32 devices in a mesh: pix: 8 (over z, x), band: 4 (over y, core).
Axes of the slice: x: 2, y: 2, z: 4, core: 2. Of those that a mesh axis runs over, the one named last changes fastest.
Arguments:
- spectra: bfloat16 [224, 32768], P('band', 'pix'), may hold values from -0.1 to 4
- endmembers: bfloat16 [224, 512], P('band'), may hold values from 0.05 to 1
- gram_inverse: float32 [512, 512], replicated, may hold values from -1 to 1, as said below
- abundances: float32 [512, 32768], P(None, ('pix', 'band')), may hold values from 0 to 512, as said below
- duals: float32 [512, 32768], P(None, ('pix', 'band')), may hold values from -4 to 4
Outputs:
- abundances_out: float32 [512, 32768], P(None, ('pix', 'band'))
- duals_out: float32 [512, 32768], P(None, ('pix', 'band'))
- residual_rms: float32 [2, 2], replicated
The draws below stay inside these ranges and needn't reach their ends.
Inputs may be any that keep to these rules, and one draw needn't show every extreme that they name: `abundances`: each column is nonnegative and sums to 512. `gram_inverse`: penalty times the float32 inverse of endmembers^T endmembers / 512^2 + penalty I, with penalty = 224 / (2 * 512^2) and the endmembers as stored.
All inputs are finite; a program needn't handle non-finite values.
Results may differ from the reference program's by a relative error of at most 0.0004.
Values may be sent and summed in bfloat16 or wider, within the bound.
No kernel may reach another device: no remote copies, remote signals or barrier semaphores. Data moves between devices by JAX's collectives and lax.ppermute only.
A program may use at most 64 MiB of HBM per device.

```python
import jax
import jax.numpy as jnp
from jax import lax

B = 224
K = 512
ITERS = 2
BISECT = 6
PIXELS = 32768


def endmember_table(key):
    return jax.random.uniform(jax.random.fold_in(key, 11), (B, K), jnp.float32, 0.05, 1.0).astype(jnp.bfloat16)


def draw_endmembers(key, part):
    return endmember_table(key)


def draw_gram_inverse(key, part):
    signatures = endmember_table(key).astype(jnp.float32)
    penalty = B / (2.0 * K * K)
    gram = jnp.dot(signatures.T, signatures, precision=lax.Precision.HIGHEST) / (K * K)
    return penalty * jnp.linalg.inv(gram + penalty * jnp.eye(K, dtype=jnp.float32))


def draw_spectra(key, part):
    signatures = endmember_table(key).astype(jnp.float32)
    logits = 2.0 * jax.random.normal(jax.random.fold_in(key, 21), (K, PIXELS), jnp.float32)
    mixing = K * jax.nn.softmax(logits, axis=0)
    position = jnp.arange(PIXELS, dtype=jnp.float32) / PIXELS
    bright = 0.6 * jnp.power(3.0, position)
    noise = jnp.clip(0.02 * jax.random.normal(jax.random.fold_in(key, 22), (B, PIXELS), jnp.float32), -0.1, 0.1)
    mixed = jnp.dot(signatures, mixing, precision=lax.Precision.HIGHEST) / K
    return (bright[None, :] * mixed + noise).astype(jnp.bfloat16)


def draw_abundances(key, part):
    logits = 1.5 * jax.random.normal(jax.random.fold_in(key, 31), (K, PIXELS), jnp.float32)
    return K * jax.nn.softmax(logits, axis=0)


def draw_duals(key, part):
    position = jnp.arange(PIXELS, dtype=jnp.float32) / PIXELS
    values = jnp.clip(jax.random.normal(jax.random.fold_in(key, 41), (K, PIXELS), jnp.float32), -4.0, 4.0)
    return 0.3 * jnp.power(3.0, position)[None, :] * values


def setup_inputs(seed: int = 0) -> dict:
    seeds = jax.random.split(jax.random.key(seed), 6)
    spectra = draw_spectra(jax.random.fold_in(seeds[5], 71), 0)
    endmembers = draw_endmembers(jax.random.fold_in(seeds[5], 71), 0)
    gram_inverse = draw_gram_inverse(jax.random.fold_in(seeds[5], 71), 0)
    abundances = draw_abundances(jax.random.fold_in(seeds[5], 71), 0)
    duals = draw_duals(jax.random.fold_in(seeds[5], 71), 0)
    return {"spectra": spectra, "endmembers": endmembers, "gram_inverse": gram_inverse, "abundances": abundances, "duals": duals}


def project(shifted):
    simplex_sum = float(K)
    high_end = lax.optimization_barrier(jnp.max(shifted, axis=0))
    low_end = (lax.optimization_barrier(jnp.sum(shifted, axis=0)) - simplex_sum) / simplex_sum

    def mass_at(level):
        return lax.optimization_barrier(jnp.sum(jnp.maximum(shifted - level[None, :], 0.0), axis=0))
    mass_low = mass_at(low_end)
    mass_high = jnp.zeros_like(high_end)

    def bisect_once(unused, state):
        low_now, high_now, low_mass, high_mass = state
        middle = 0.5 * (low_now + high_now)
        total_mass = mass_at(middle)
        too_high = total_mass > simplex_sum
        return (jnp.where(too_high, middle, low_now), jnp.where(too_high, high_now, middle), jnp.where(too_high, total_mass, low_mass), jnp.where(too_high, high_mass, total_mass))
    low_end, high_end, mass_low, mass_high = lax.fori_loop(0, BISECT, bisect_once, (low_end, high_end, mass_low, mass_high))
    level = low_end + (mass_low - simplex_sum) * (high_end - low_end) / (mass_low - mass_high)
    return jnp.maximum(shifted - level[None, :], 0.0)

def reference(spectra, endmembers, gram_inverse, abundances, duals):
    penalty = B / (2.0 * K * K)
    fit_term = jnp.dot(endmembers.T.astype(jnp.float32), spectra.astype(jnp.float32), preferred_element_type=jnp.float32) / K
    current = abundances
    scaled_dual = duals
    primal_list = []
    change_list = []
    for sweep in range(ITERS):
        primal = jnp.dot(gram_inverse, fit_term / penalty + current - scaled_dual, precision=lax.Precision.HIGHEST)
        updated = project(primal + scaled_dual)
        scaled_dual = scaled_dual + primal - updated
        primal_list.append(jnp.sum((primal - updated) ** 2))
        change_list.append(jnp.sum((updated - current) ** 2))
        current = updated
    totals = jnp.stack([jnp.stack(primal_list), jnp.stack(change_list)])
    residual_rms = jnp.sqrt(totals / PIXELS)
    return (current, scaled_dual, residual_rms)
```

```python
import functools

import jax
import jax.numpy as jnp
from jax import lax
from jax.experimental import pallas as pl
from jax.experimental.pallas import tpu as pltpu
from jax.sharding import PartitionSpec as P

B = 224
K = 512
ITERS = 2
BISECT = 6
ROWS = 8
PACK = 16
LANES = 128


def dot(left, right):
    return lax.dot_general(
        left, right, (((1,), (0,)), ((), ())), preferred_element_type=jnp.float32
    )


def dot_rows(left, right):
    return lax.dot_general(
        left, right, (((1,), (1,)), ((), ())), preferred_element_type=jnp.float32
    )


def halves(value):
    high = value.astype(jnp.bfloat16)
    return high, (value - high.astype(jnp.float32)).astype(jnp.bfloat16)


def prepare_kernel(blocks, *refs):
    gram_ref, z_ref, u_ref = refs[:3]
    member_refs = refs[3 : 3 + blocks]
    start_ref, gh_ref, gl_ref, wh_ref, wl_ref, rows_ref = refs[3 + blocks :]
    scale = 1.0 / (K * (B / (2.0 * K * K)))
    gram = gram_ref[...]
    gh = gram.astype(jnp.bfloat16)
    rest = gram - gh.astype(jnp.float32)
    gl = rest.astype(jnp.bfloat16)
    g3 = (rest - gl.astype(jnp.float32)).astype(jnp.bfloat16)
    gh_ref[...] = gh
    gl_ref[...] = gl
    depth = member_refs[0].shape[0]
    for k, ref in enumerate(member_refs):
        rows_ref[k * depth : (k + 1) * depth, :] = ref[...].astype(jnp.float32)
    members = rows_ref[...].astype(jnp.bfloat16)
    weights = (dot_rows(g3, members) + dot_rows(gl, members)) + dot_rows(gh, members)
    wh, wl = halves(weights * scale)
    wh_ref[...] = wh
    wl_ref[...] = wl
    width = z_ref.shape[1]
    step = min(width, 256)
    for j in range(0, width, step):
        columns = slice(j, j + step)
        dual = u_ref[:, columns]
        high, low = halves(z_ref[:, columns] - dual)
        product = dot(gh, high) + (dot(gh, low) + dot(gl, high))
        start_ref[:, columns] = product + dual


def mass_of(v_ref, level):
    width = level.shape[1]
    wide = jnp.broadcast_to(level, (ROWS, width))
    total = jnp.zeros((ROWS, width), jnp.float32)
    for r in range(0, K, ROWS):
        total = total + jnp.maximum(v_ref[r : r + ROWS, :], wide)
    return jnp.sum(total, axis=0, keepdims=True) - float(K) * level


def threshold(v_ref, total, high_end):
    simplex_sum = float(K)
    low_end = (total - simplex_sum) / simplex_sum
    mass_low = mass_of(v_ref, low_end)
    mass_high = jnp.zeros_like(high_end)

    def bisect_once(unused, state):
        low_now, high_now, low_mass, high_mass = state
        middle = 0.5 * (low_now + high_now)
        mass = mass_of(v_ref, middle)
        too_high = mass > simplex_sum
        return (
            jnp.where(too_high, middle, low_now),
            jnp.where(too_high, high_now, middle),
            jnp.where(too_high, mass, low_mass),
            jnp.where(too_high, high_mass, mass),
        )

    low_end, high_end, mass_low, mass_high = lax.fori_loop(
        0, BISECT, bisect_once, (low_end, high_end, mass_low, mass_high)
    )
    return low_end + (mass_low - simplex_sum) * (high_end - low_end) / (mass_low - mass_high)


def fold(value):
    total = value[:, :LANES]
    for j in range(LANES, value.shape[1], LANES):
        total = total + value[:, j : j + LANES]
    return jnp.sum(total, axis=0, keepdims=True)


def column_stats(v_ref, columns):
    block = v_ref[0:ROWS, columns]
    total = block
    top = block
    for r in range(ROWS, K, ROWS):
        block = v_ref[r : r + ROWS, columns]
        total = total + block
        top = jnp.maximum(top, block)
    return jnp.sum(total, axis=0, keepdims=True), jnp.max(top, axis=0, keepdims=True)


def admm_kernel(blocks, copies, *refs):
    start_ref, gh_ref, gl_ref, wh_ref, wl_ref = refs[:5]
    spectra_refs = refs[5 : 5 + blocks]
    z_hbm, u_hbm = refs[5 + blocks : 7 + blocks]
    z_out, u_out, sums_ref = refs[7 + blocks : 10 + blocks]
    rows_ref, z_ref, u_ref, v_ref, v2_ref, high_ref, low_ref, in_sems, out_sems = refs[10 + blocks :]
    load_z = pltpu.make_async_copy(z_hbm, z_ref, in_sems.at[0])
    load_u = pltpu.make_async_copy(u_hbm, u_ref, in_sems.at[1])
    load_z.start()
    load_u.start()
    width = v_ref.shape[1]
    step = min(width, 256)
    depth = spectra_refs[0].shape[0]
    for k, ref in enumerate(spectra_refs):
        rows_ref[k * depth : (k + 1) * depth, :] = ref[...].astype(jnp.float32)
    stats = []
    for j in range(0, width, step):
        columns = slice(j, j + step)
        pixels = rows_ref[:, columns].astype(jnp.bfloat16)
        v_ref[:, columns] = (dot(wl_ref[...], pixels) + dot(wh_ref[...], pixels)) + start_ref[:, columns]
        stats.append(column_stats(v_ref, columns))
    total = jnp.concatenate([s for s, _ in stats], axis=1)
    top = jnp.concatenate([t for _, t in stats], axis=1)
    level = threshold(v_ref, total, top)
    load_z.wait()
    load_u.wait()
    wide = jnp.broadcast_to(level, (ROWS, width))
    primal1 = jnp.zeros((ROWS, width), jnp.float32)
    change1 = primal1
    for r in range(0, K, PACK):
        pieces = []
        for q in (r, r + ROWS):
            rows = slice(q, q + ROWS)
            v = v_ref[rows, :]
            z = jnp.maximum(v - wide, 0.0)
            u = jnp.minimum(v, wide)
            du = u - u_ref[rows, :]
            dz = z - z_ref[rows, :]
            primal1 = primal1 + du * du
            change1 = change1 + dz * dz
            pieces.append(z - u)
        high, low = halves(jnp.concatenate(pieces, axis=0))
        high_ref[r : r + PACK, :] = high
        low_ref[r : r + PACK, :] = low
    stats = []
    for j in range(0, width, step):
        columns = slice(j, j + step)
        high = high_ref[:, columns]
        product = dot(gh_ref[...], high) + (dot(gh_ref[...], low_ref[:, columns]) + dot(gl_ref[...], high))
        v = v_ref[:, columns]
        v2_ref[:, columns] = product + ((v - start_ref[:, columns]) + jnp.minimum(v, level[:, columns]))
        stats.append(column_stats(v2_ref, columns))
    total = jnp.concatenate([s for s, _ in stats], axis=1)
    top = jnp.concatenate([t for _, t in stats], axis=1)
    level2 = threshold(v2_ref, total, top)
    wide2 = jnp.broadcast_to(level2, (ROWS, width))
    primal2 = jnp.zeros((ROWS, width), jnp.float32)
    change2 = primal2
    part = K // copies
    stores = []
    for c in range(copies):
        for r in range(c * part, (c + 1) * part, ROWS):
            rows = slice(r, r + ROWS)
            v = v_ref[rows, :]
            v2 = v2_ref[rows, :]
            z2 = jnp.maximum(v2 - wide2, 0.0)
            u2 = jnp.minimum(v2, wide2)
            du = u2 - jnp.minimum(v, wide)
            dz = z2 - jnp.maximum(v - wide, 0.0)
            primal2 = primal2 + du * du
            change2 = change2 + dz * dz
            z_ref[rows, :] = z2
            u_ref[rows, :] = u2
        rows = pl.ds(c * part, part)
        for side, (source, target) in enumerate(((z_ref, z_out), (u_ref, u_out))):
            store = pltpu.make_async_copy(source.at[rows, :], target.at[rows, :], out_sems.at[side, c])
            store.start()
            stores.append(store)
    lane = lax.broadcasted_iota(jnp.int32, (1, LANES), 1)
    line = jnp.zeros((1, LANES), jnp.float32)
    for i, value in enumerate((primal1, primal2, change1, change2)):
        whole = jnp.sum(fold(value), axis=1, keepdims=True)
        line = jnp.where(lane == i, whole, line)
    sums_ref[...] = jnp.broadcast_to(line, sums_ref.shape)
    for store in stores:
        store.wait()


def finish_kernel(pixel_count, sums_ref, out_ref):
    total = jnp.sum(sums_ref[...], axis=0, keepdims=True)
    root = jnp.sqrt(total / pixel_count)
    lane = lax.broadcasted_iota(jnp.int32, (1, LANES), 1)
    values = [jnp.sum(jnp.where(lane == i, root, 0.0), axis=1, keepdims=True) for i in range(4)]
    row = lax.broadcasted_iota(jnp.int32, (2, 2), 0)
    column = lax.broadcasted_iota(jnp.int32, (2, 2), 1)
    out = jnp.zeros((2, 2), jnp.float32)
    for i in range(4):
        out = jnp.where((row == i // 2) & (column == i % 2), values[i], out)
    out_ref[...] = out


def body(sizes, spectra, endmembers, gram_inverse, abundances, duals):
    n_pix, n_band = sizes
    width = abundances.shape[1]
    depth = spectra.shape[0]
    me = lax.axis_index("band")

    def partner(i, k):
        return i ^ k if n_band & (n_band - 1) == 0 else (i + k) % n_band

    def send(x, k):
        return lax.ppermute(x, "band", [(i, partner(i, k)) for i in range(n_band)])

    members = [endmembers] + [None] * (n_band - 1)
    if n_band & (n_band - 1) == 0:
        stride = n_band // 2
        have = [0]
        while stride:
            for h in list(have):
                members[h ^ stride] = send(members[h], stride)
                have.append(h ^ stride)
            stride //= 2
    else:
        for k in range(1, n_band):
            members[k] = send(endmembers, k)
    pixels = []
    for k in range(n_band):
        block = lax.dynamic_slice(spectra, (0, partner(me, k) * width), (depth, width))
        pixels.append(send(block, k) if k else block)

    vmem = pl.BlockSpec(memory_space=pltpu.VMEM)
    anywhere = pl.BlockSpec(memory_space=pl.ANY)
    f32 = jnp.float32
    bf16 = jnp.bfloat16
    start, gh, gl, wh, wl = pl.pallas_call(
        functools.partial(prepare_kernel, n_band),
        out_shape=(
            jax.ShapeDtypeStruct((K, width), f32),
            jax.ShapeDtypeStruct((K, K), bf16),
            jax.ShapeDtypeStruct((K, K), bf16),
            jax.ShapeDtypeStruct((K, n_band * depth), bf16),
            jax.ShapeDtypeStruct((K, n_band * depth), bf16),
        ),
        in_specs=[vmem] * (3 + n_band),
        out_specs=(vmem,) * 5,
        scratch_shapes=[pltpu.VMEM((n_band * depth, K), f32)],
        compiler_params=pltpu.CompilerParams(vmem_limit_bytes=20 << 20),
        cost_estimate=pl.CostEstimate(flops=12 * K * K * width, transcendentals=0, bytes_accessed=8 * K * width),
        name="prepare",
    )(gram_inverse, abundances, duals, *members)
    copies = 4
    z, u, sums = pl.pallas_call(
        functools.partial(admm_kernel, n_band, copies),
        out_shape=(
            jax.ShapeDtypeStruct((K, width), f32),
            jax.ShapeDtypeStruct((K, width), f32),
            jax.ShapeDtypeStruct((n_pix * n_band, LANES), f32),
        ),
        in_specs=[vmem] * (5 + n_band) + [anywhere] * 2,
        out_specs=(anywhere, anywhere, vmem),
        scratch_shapes=[
            pltpu.VMEM((n_band * depth, width), f32),
            pltpu.VMEM((K, width), f32),
            pltpu.VMEM((K, width), f32),
            pltpu.VMEM((K, width), f32),
            pltpu.VMEM((K, width), f32),
            pltpu.VMEM((K, width), bf16),
            pltpu.VMEM((K, width), bf16),
            pltpu.SemaphoreType.DMA((2,)),
            pltpu.SemaphoreType.DMA((2, copies)),
        ],
        compiler_params=pltpu.CompilerParams(vmem_limit_bytes=32 << 20),
        cost_estimate=pl.CostEstimate(flops=12 * K * K * width, transcendentals=0, bytes_accessed=16 * K * width),
        name="admm",
    )(start, gh, gl, wh, wl, *pixels, abundances, duals)
    everyone = lax.all_to_all(sums, ("pix", "band"), 0, 0, tiled=True)
    residual_rms = pl.pallas_call(
        functools.partial(finish_kernel, float(width * n_pix * n_band)),
        out_shape=jax.ShapeDtypeStruct((2, 2), f32),
        in_specs=[vmem],
        out_specs=vmem,
        name="finish",
    )(everyone)
    return (z, u, residual_rms)


def solution(mesh):
    sizes = (mesh.shape["pix"], mesh.shape["band"])
    return jax.shard_map(
        functools.partial(body, sizes),
        mesh=mesh,
        in_specs=(
            P("band", "pix"),
            P("band", None),
            P(),
            P(None, ("pix", "band")),
            P(None, ("pix", "band")),
        ),
        out_specs=(P(None, ("pix", "band")), P(None, ("pix", "band")), P()),
        check_vma=False,
    )
```

```python
import functools

import jax
import jax.numpy as jnp
from jax import lax
from jax.experimental import pallas as pl
from jax.experimental.pallas import tpu as pltpu
from jax.sharding import PartitionSpec as P

B = 224
K = 512
ITERS = 2
BISECT = 6
ROWS = 8
PACK = 16
LANES = 128


def dot(left, right):
    return lax.dot_general(
        left, right, (((1,), (0,)), ((), ())), preferred_element_type=jnp.float32
    )


def dot_rows(left, right):
    return lax.dot_general(
        left, right, (((1,), (1,)), ((), ())), preferred_element_type=jnp.float32
    )


def halves(value):
    high = value.astype(jnp.bfloat16)
    return high, (value - high.astype(jnp.float32)).astype(jnp.bfloat16)


def gram_kernel(gram_hbm, z_hbm, u_hbm, start_ref, gh_ref, gl_ref, g3_ref, gram_ref, z_ref, u_ref, gram_sem, sems):
    width = z_ref.shape[1]
    step = min(width, 256)
    load_gram = pltpu.make_async_copy(gram_hbm, gram_ref, gram_sem)
    load_gram.start()
    loads = []
    for i, j in enumerate(range(0, width, step)):
        columns = pl.ds(j, step)
        pair = (
            pltpu.make_async_copy(z_hbm.at[:, columns], z_ref.at[:, columns], sems.at[0, i]),
            pltpu.make_async_copy(u_hbm.at[:, columns], u_ref.at[:, columns], sems.at[1, i]),
        )
        for load in pair:
            load.start()
        loads.append(pair)
    load_gram.wait()
    gram = gram_ref[...]
    gh = gram.astype(jnp.bfloat16)
    rest = gram - gh.astype(jnp.float32)
    gl = rest.astype(jnp.bfloat16)
    gh_ref[...] = gh
    gl_ref[...] = gl
    g3_ref[...] = (rest - gl.astype(jnp.float32)).astype(jnp.bfloat16)
    for i, j in enumerate(range(0, width, step)):
        for load in loads[i]:
            load.wait()
        columns = slice(j, j + step)
        dual = u_ref[:, columns]
        high, low = halves(z_ref[:, columns] - dual)
        product = dot(gh, high) + (dot(gh, low) + dot(gl, high))
        start_ref[:, columns] = product + dual


def weights_kernel(blocks, *refs):
    gh_ref, gl_ref, g3_ref = refs[:3]
    member_refs = refs[3 : 3 + blocks]
    wh_ref, wl_ref, rows_ref = refs[3 + blocks :]
    scale = 1.0 / (K * (B / (2.0 * K * K)))
    depth = member_refs[0].shape[0]
    for k, ref in enumerate(member_refs):
        rows_ref[k * depth : (k + 1) * depth, :] = ref[...].astype(jnp.float32)
    members = rows_ref[...].astype(jnp.bfloat16)
    weights = (dot_rows(g3_ref[...], members) + dot_rows(gl_ref[...], members)) + dot_rows(gh_ref[...], members)
    wh, wl = halves(weights * scale)
    wh_ref[...] = wh
    wl_ref[...] = wl


def mass_of(v_ref, level):
    width = level.shape[1]
    wide = jnp.broadcast_to(level, (ROWS, width))
    total = jnp.zeros((ROWS, width), jnp.float32)
    for r in range(0, K, ROWS):
        total = total + jnp.maximum(v_ref[r : r + ROWS, :], wide)
    return jnp.sum(total, axis=0, keepdims=True) - float(K) * level


def threshold(v_ref, total, high_end):
    simplex_sum = float(K)
    low_end = (total - simplex_sum) / simplex_sum
    mass_low = mass_of(v_ref, low_end)
    mass_high = jnp.zeros_like(high_end)

    def bisect_once(unused, state):
        low_now, high_now, low_mass, high_mass = state
        middle = 0.5 * (low_now + high_now)
        mass = mass_of(v_ref, middle)
        too_high = mass > simplex_sum
        return (
            jnp.where(too_high, middle, low_now),
            jnp.where(too_high, high_now, middle),
            jnp.where(too_high, mass, low_mass),
            jnp.where(too_high, high_mass, mass),
        )

    low_end, high_end, mass_low, mass_high = lax.fori_loop(
        0, BISECT, bisect_once, (low_end, high_end, mass_low, mass_high)
    )
    return low_end + (mass_low - simplex_sum) * (high_end - low_end) / (mass_low - mass_high)


def fold(value):
    total = value[:, :LANES]
    for j in range(LANES, value.shape[1], LANES):
        total = total + value[:, j : j + LANES]
    return jnp.sum(total, axis=0, keepdims=True)


def column_stats(v_ref, columns):
    block = v_ref[0:ROWS, columns]
    total = block
    top = block
    for r in range(ROWS, K, ROWS):
        block = v_ref[r : r + ROWS, columns]
        total = total + block
        top = jnp.maximum(top, block)
    return jnp.sum(total, axis=0, keepdims=True), jnp.max(top, axis=0, keepdims=True)


def admm_kernel(blocks, *refs):
    start_ref, gh_ref, gl_ref, wh_ref, wl_ref = refs[:5]
    spectra_refs = refs[5 : 5 + blocks]
    z_hbm, u_hbm = refs[5 + blocks : 7 + blocks]
    z_out, u_out, sums_ref = refs[7 + blocks : 10 + blocks]
    rows_ref, z_ref, u_ref, v_ref, v2_ref, high_ref, low_ref, in_sems = refs[10 + blocks :]
    load_z = pltpu.make_async_copy(z_hbm, z_ref, in_sems.at[0])
    load_u = pltpu.make_async_copy(u_hbm, u_ref, in_sems.at[1])
    load_z.start()
    load_u.start()
    width = v_ref.shape[1]
    step = min(width, 256)
    depth = spectra_refs[0].shape[0]
    for k, ref in enumerate(spectra_refs):
        rows_ref[k * depth : (k + 1) * depth, :] = ref[...].astype(jnp.float32)
    stats = []
    for j in range(0, width, step):
        columns = slice(j, j + step)
        pixels = rows_ref[:, columns].astype(jnp.bfloat16)
        v_ref[:, columns] = (dot(wl_ref[...], pixels) + dot(wh_ref[...], pixels)) + start_ref[:, columns]
        stats.append(column_stats(v_ref, columns))
    total = jnp.concatenate([s for s, _ in stats], axis=1)
    top = jnp.concatenate([t for _, t in stats], axis=1)
    level = threshold(v_ref, total, top)
    load_z.wait()
    load_u.wait()
    wide = jnp.broadcast_to(level, (ROWS, width))
    primal1 = jnp.zeros((ROWS, width), jnp.float32)
    change1 = primal1
    for r in range(0, K, PACK):
        pieces = []
        for q in (r, r + ROWS):
            rows = slice(q, q + ROWS)
            v = v_ref[rows, :]
            z = jnp.maximum(v - wide, 0.0)
            u = jnp.minimum(v, wide)
            du = u - u_ref[rows, :]
            dz = z - z_ref[rows, :]
            primal1 = primal1 + du * du
            change1 = change1 + dz * dz
            pieces.append(z - u)
        high, low = halves(jnp.concatenate(pieces, axis=0))
        high_ref[r : r + PACK, :] = high
        low_ref[r : r + PACK, :] = low
    stats = []
    for j in range(0, width, step):
        columns = slice(j, j + step)
        high = high_ref[:, columns]
        product = dot(gh_ref[...], high) + (dot(gh_ref[...], low_ref[:, columns]) + dot(gl_ref[...], high))
        v = v_ref[:, columns]
        v2_ref[:, columns] = product + ((v - start_ref[:, columns]) + jnp.minimum(v, level[:, columns]))
        stats.append(column_stats(v2_ref, columns))
    total = jnp.concatenate([s for s, _ in stats], axis=1)
    top = jnp.concatenate([t for _, t in stats], axis=1)
    level2 = threshold(v2_ref, total, top)
    wide2 = jnp.broadcast_to(level2, (ROWS, width))
    primal2 = jnp.zeros((ROWS, width), jnp.float32)
    change2 = primal2
    for r in range(0, K, ROWS):
        rows = slice(r, r + ROWS)
        v = v_ref[rows, :]
        v2 = v2_ref[rows, :]
        z2 = jnp.maximum(v2 - wide2, 0.0)
        u2 = jnp.minimum(v2, wide2)
        du = u2 - jnp.minimum(v, wide)
        dz = z2 - jnp.maximum(v - wide, 0.0)
        primal2 = primal2 + du * du
        change2 = change2 + dz * dz
        z_out[rows, :] = z2
        u_out[rows, :] = u2
    lane = lax.broadcasted_iota(jnp.int32, (1, LANES), 1)
    line = jnp.zeros((1, LANES), jnp.float32)
    for i, value in enumerate((primal1, primal2, change1, change2)):
        whole = jnp.sum(fold(value), axis=1, keepdims=True)
        line = jnp.where(lane == i, whole, line)
    sums_ref[...] = jnp.broadcast_to(line, sums_ref.shape)


def finish_kernel(pixel_count, sums_ref, out_ref):
    total = jnp.sum(sums_ref[...], axis=0, keepdims=True)
    root = jnp.sqrt(total / pixel_count)
    lane = lax.broadcasted_iota(jnp.int32, (1, LANES), 1)
    values = [jnp.sum(jnp.where(lane == i, root, 0.0), axis=1, keepdims=True) for i in range(4)]
    row = lax.broadcasted_iota(jnp.int32, (2, 2), 0)
    column = lax.broadcasted_iota(jnp.int32, (2, 2), 1)
    out = jnp.zeros((2, 2), jnp.float32)
    for i in range(4):
        out = jnp.where((row == i // 2) & (column == i % 2), values[i], out)
    out_ref[...] = out


def body(sizes, spectra, endmembers, gram_inverse, abundances, duals):
    n_pix, n_band = sizes
    width = abundances.shape[1]
    depth = spectra.shape[0]
    me = lax.axis_index("band")

    def partner(i, k):
        return i ^ k if n_band & (n_band - 1) == 0 else (i + k) % n_band

    def send(x, k):
        return lax.ppermute(x, "band", [(i, partner(i, k)) for i in range(n_band)])

    members = [endmembers] + [None] * (n_band - 1)
    if n_band & (n_band - 1) == 0:
        stride = n_band // 2
        have = [0]
        while stride:
            for h in list(have):
                members[h ^ stride] = send(members[h], stride)
                have.append(h ^ stride)
            stride //= 2
    else:
        for k in range(1, n_band):
            members[k] = send(endmembers, k)
    pixels = []
    for k in range(n_band):
        block = lax.dynamic_slice(spectra, (0, partner(me, k) * width), (depth, width))
        pixels.append(send(block, k) if k else block)

    vmem = pl.BlockSpec(memory_space=pltpu.VMEM)
    hbm = pl.BlockSpec(memory_space=pltpu.HBM)
    f32 = jnp.float32
    bf16 = jnp.bfloat16
    gram_inverse, abundances, duals = (
        pltpu.with_memory_space_constraint(x, pltpu.HBM) for x in (gram_inverse, abundances, duals)
    )
    step = min(width, 256)
    start, gh, gl, g3 = pl.pallas_call(
        gram_kernel,
        out_shape=(jax.ShapeDtypeStruct((K, width), f32),) + (jax.ShapeDtypeStruct((K, K), bf16),) * 3,
        in_specs=[hbm] * 3,
        out_specs=(vmem,) * 4,
        scratch_shapes=[
            pltpu.VMEM((K, K), f32),
            pltpu.VMEM((K, width), f32),
            pltpu.VMEM((K, width), f32),
            pltpu.SemaphoreType.DMA,
            pltpu.SemaphoreType.DMA((2, width // step)),
        ],
        compiler_params=pltpu.CompilerParams(vmem_limit_bytes=20 << 20),
        cost_estimate=pl.CostEstimate(flops=12 * K * K * width, transcendentals=0, bytes_accessed=8 * K * width),
        name="gram",
    )(gram_inverse, abundances, duals)
    wh, wl = pl.pallas_call(
        functools.partial(weights_kernel, n_band),
        out_shape=(jax.ShapeDtypeStruct((K, n_band * depth), bf16),) * 2,
        in_specs=[vmem] * (3 + n_band),
        out_specs=(vmem,) * 2,
        scratch_shapes=[pltpu.VMEM((n_band * depth, K), f32)],
        compiler_params=pltpu.CompilerParams(vmem_limit_bytes=8 << 20),
        cost_estimate=pl.CostEstimate(flops=6 * K * K * n_band * depth, transcendentals=0, bytes_accessed=4 * K * K),
        name="weights",
    )(gh, gl, g3, *members)
    z, u, sums = pl.pallas_call(
        functools.partial(admm_kernel, n_band),
        out_shape=(
            jax.ShapeDtypeStruct((K, width), f32),
            jax.ShapeDtypeStruct((K, width), f32),
            jax.ShapeDtypeStruct((n_pix * n_band, LANES), f32),
        ),
        in_specs=[vmem] * (5 + n_band) + [hbm] * 2,
        out_specs=(vmem,) * 3,
        scratch_shapes=[
            pltpu.VMEM((n_band * depth, width), f32),
            pltpu.VMEM((K, width), f32),
            pltpu.VMEM((K, width), f32),
            pltpu.VMEM((K, width), f32),
            pltpu.VMEM((K, width), f32),
            pltpu.VMEM((K, width), bf16),
            pltpu.VMEM((K, width), bf16),
            pltpu.SemaphoreType.DMA((2,)),
        ],
        compiler_params=pltpu.CompilerParams(vmem_limit_bytes=32 << 20),
        cost_estimate=pl.CostEstimate(flops=12 * K * K * width, transcendentals=0, bytes_accessed=16 * K * width),
        name="admm",
    )(start, gh, gl, wh, wl, *pixels, abundances, duals)
    everyone = lax.all_to_all(sums, ("pix", "band"), 0, 0, tiled=True)
    residual_rms = pl.pallas_call(
        functools.partial(finish_kernel, float(width * n_pix * n_band)),
        out_shape=jax.ShapeDtypeStruct((2, 2), f32),
        in_specs=[vmem],
        out_specs=vmem,
        name="finish",
    )(everyone)
    return (z, u, residual_rms)


def solution(mesh):
    sizes = (mesh.shape["pix"], mesh.shape["band"])
    return jax.shard_map(
        functools.partial(body, sizes),
        mesh=mesh,
        in_specs=(
            P("band", "pix"),
            P("band", None),
            P(),
            P(None, ("pix", "band")),
            P(None, ("pix", "band")),
        ),
        out_specs=(P(None, ("pix", "band")), P(None, ("pix", "band")), P()),
        check_vma=False,
    )
```

```python
import functools

import jax
import jax.numpy as jnp
from jax import lax
from jax.experimental import pallas as pl
from jax.experimental.pallas import tpu as pltpu
from jax.sharding import PartitionSpec as P

B = 224
K = 512
ITERS = 2
BISECT = 6
ROWS = 8
PACK = 16
LANES = 128


def dot(left, right):
    return lax.dot_general(
        left, right, (((1,), (0,)), ((), ())), preferred_element_type=jnp.float32
    )


def dot_rows(left, right):
    return lax.dot_general(
        left, right, (((1,), (1,)), ((), ())), preferred_element_type=jnp.float32
    )


def halves(value):
    high = value.astype(jnp.bfloat16)
    return high, (value - high.astype(jnp.float32)).astype(jnp.bfloat16)


def slice_kernel(offsets, spectra_ref, *refs):
    outs, sems = refs[:-1], refs[-1]
    width = outs[0].shape[1]
    copies = []
    for i, (offset, out) in enumerate(zip(offsets(), outs)):
        columns = pl.ds(pl.multiple_of(offset * width, LANES), width)
        copies.append(pltpu.make_async_copy(spectra_ref.at[:, columns], out, sems.at[i]))
    for copy in copies:
        copy.start()
    for copy in copies:
        copy.wait()


def gram_kernel(gram_ref, z_ref, u_ref, start_ref, gh_ref, gl_ref, g3_ref):
    width = z_ref.shape[1]
    step = min(width, 256)
    gram = gram_ref[...]
    gh = gram.astype(jnp.bfloat16)
    rest = gram - gh.astype(jnp.float32)
    gl = rest.astype(jnp.bfloat16)
    gh_ref[...] = gh
    gl_ref[...] = gl
    g3_ref[...] = (rest - gl.astype(jnp.float32)).astype(jnp.bfloat16)
    for j in range(0, width, step):
        columns = slice(j, j + step)
        dual = u_ref[:, columns]
        high, low = halves(z_ref[:, columns] - dual)
        product = dot(gh_ref[...], high) + (dot(gh_ref[...], low) + dot(gl_ref[...], high))
        start_ref[:, columns] = product + dual


def weights_kernel(blocks, *refs):
    gh_ref, gl_ref, g3_ref = refs[:3]
    member_refs = refs[3 : 3 + blocks]
    wh_ref, wl_ref, rows_ref = refs[3 + blocks :]
    scale = 1.0 / (K * (B / (2.0 * K * K)))
    depth = member_refs[0].shape[0]
    for k, ref in enumerate(member_refs):
        rows_ref[k * depth : (k + 1) * depth, :] = ref[...].astype(jnp.float32)
    members = rows_ref[...].astype(jnp.bfloat16)
    weights = (dot_rows(g3_ref[...], members) + dot_rows(gl_ref[...], members)) + dot_rows(gh_ref[...], members)
    wh, wl = halves(weights * scale)
    wh_ref[...] = wh
    wl_ref[...] = wl


def mass_of(v_ref, level):
    width = level.shape[1]
    wide = jnp.broadcast_to(level, (ROWS, width))
    total = jnp.zeros((ROWS, width), jnp.float32)
    for r in range(0, K, ROWS):
        total = total + jnp.maximum(v_ref[r : r + ROWS, :], wide)
    return jnp.sum(total, axis=0, keepdims=True) - float(K) * level


def threshold(v_ref, total, high_end):
    simplex_sum = float(K)
    low_end = (total - simplex_sum) / simplex_sum
    mass_low = mass_of(v_ref, low_end)
    mass_high = jnp.zeros_like(high_end)

    def bisect_once(unused, state):
        low_now, high_now, low_mass, high_mass = state
        middle = 0.5 * (low_now + high_now)
        mass = mass_of(v_ref, middle)
        too_high = mass > simplex_sum
        return (
            jnp.where(too_high, middle, low_now),
            jnp.where(too_high, high_now, middle),
            jnp.where(too_high, mass, low_mass),
            jnp.where(too_high, high_mass, mass),
        )

    low_end, high_end, mass_low, mass_high = lax.fori_loop(
        0, BISECT, bisect_once, (low_end, high_end, mass_low, mass_high)
    )
    return low_end + (mass_low - simplex_sum) * (high_end - low_end) / (mass_low - mass_high)


def fold(value):
    total = value[:, :LANES]
    for j in range(LANES, value.shape[1], LANES):
        total = total + value[:, j : j + LANES]
    return jnp.sum(total, axis=0, keepdims=True)


def column_stats(v_ref, columns):
    block = v_ref[0:ROWS, columns]
    total = block
    top = block
    for r in range(ROWS, K, ROWS):
        block = v_ref[r : r + ROWS, columns]
        total = total + block
        top = jnp.maximum(top, block)
    return jnp.sum(total, axis=0, keepdims=True), jnp.max(top, axis=0, keepdims=True)


def admm_kernel(blocks, *refs):
    start_ref, gh_ref, gl_ref, wh_ref, wl_ref = refs[:5]
    spectra_refs = refs[5 : 5 + blocks]
    z_ref, u_ref = refs[5 + blocks : 7 + blocks]
    z_out, u_out, sums_ref = refs[7 + blocks : 10 + blocks]
    rows_ref, v_ref, v2_ref, high_ref, low_ref = refs[10 + blocks :]
    width = v_ref.shape[1]
    step = min(width, 256)
    depth = spectra_refs[0].shape[0]
    for k, ref in enumerate(spectra_refs):
        rows_ref[k * depth : (k + 1) * depth, :] = ref[...].astype(jnp.float32)
    stats = []
    for j in range(0, width, step):
        columns = slice(j, j + step)
        pixels = rows_ref[:, columns].astype(jnp.bfloat16)
        v_ref[:, columns] = (dot(wl_ref[...], pixels) + dot(wh_ref[...], pixels)) + start_ref[:, columns]
        stats.append(column_stats(v_ref, columns))
    total = jnp.concatenate([s for s, _ in stats], axis=1)
    top = jnp.concatenate([t for _, t in stats], axis=1)
    level = threshold(v_ref, total, top)
    wide = jnp.broadcast_to(level, (ROWS, width))
    primal1 = jnp.zeros((ROWS, width), jnp.float32)
    change1 = primal1
    for r in range(0, K, PACK):
        pieces = []
        for q in (r, r + ROWS):
            rows = slice(q, q + ROWS)
            v = v_ref[rows, :]
            u = jnp.minimum(v, wide)
            z = v - u
            du = u - u_ref[rows, :]
            dz = z - z_ref[rows, :]
            primal1 = primal1 + du * du
            change1 = change1 + dz * dz
            pieces.append(z - u)
        high, low = halves(jnp.concatenate(pieces, axis=0))
        high_ref[r : r + PACK, :] = high
        low_ref[r : r + PACK, :] = low
    stats = []
    for j in range(0, width, step):
        columns = slice(j, j + step)
        high = high_ref[:, columns]
        product = dot(gh_ref[...], high) + (dot(gh_ref[...], low_ref[:, columns]) + dot(gl_ref[...], high))
        v = v_ref[:, columns]
        v2_ref[:, columns] = product + ((v - start_ref[:, columns]) + jnp.minimum(v, level[:, columns]))
        stats.append(column_stats(v2_ref, columns))
    total = jnp.concatenate([s for s, _ in stats], axis=1)
    top = jnp.concatenate([t for _, t in stats], axis=1)
    level2 = threshold(v2_ref, total, top)
    wide2 = jnp.broadcast_to(level2, (ROWS, width))
    primal2 = jnp.zeros((ROWS, width), jnp.float32)
    change2 = primal2
    for r in range(0, K, ROWS):
        rows = slice(r, r + ROWS)
        v = v_ref[rows, :]
        v2 = v2_ref[rows, :]
        u2 = jnp.minimum(v2, wide2)
        du = u2 - jnp.minimum(v, wide)
        dz = (v2 - v) - du
        primal2 = primal2 + du * du
        change2 = change2 + dz * dz
        z_out[rows, :] = v2 - u2
        u_out[rows, :] = u2
    row = lax.broadcasted_iota(jnp.int32, sums_ref.shape, 1)
    column = lax.broadcasted_iota(jnp.int32, sums_ref.shape, 2)
    sums = jnp.zeros(sums_ref.shape, jnp.float32)
    for i, value in enumerate((primal1, primal2, change1, change2)):
        whole = jnp.sum(fold(value), axis=1, keepdims=True)
        sums = jnp.where((row == i // 2) & (column == i % 2), whole[None], sums)
    sums_ref[...] = sums


def body(sizes, spectra, endmembers, gram_inverse, abundances, duals):
    n_pix, n_band = sizes
    width = abundances.shape[1]
    depth = spectra.shape[0]

    def partner(i, k):
        return i ^ k if n_band & (n_band - 1) == 0 else (i + k) % n_band

    def send(x, k):
        return lax.ppermute(x, "band", [(i, partner(i, k)) for i in range(n_band)])

    members = [endmembers] + [None] * (n_band - 1)
    if n_band & (n_band - 1) == 0:
        stride = n_band // 2
        have = [0]
        while stride:
            for h in list(have):
                members[h ^ stride] = send(members[h], stride)
                have.append(h ^ stride)
            stride //= 2
    else:
        for k in range(1, n_band):
            members[k] = send(endmembers, k)
    vmem = pl.BlockSpec(memory_space=pltpu.VMEM)
    hbm = pl.BlockSpec(memory_space=pltpu.HBM)
    f32 = jnp.float32
    bf16 = jnp.bfloat16
    blocks = pl.pallas_call(
        functools.partial(slice_kernel, lambda: [partner(lax.axis_index("band"), k) for k in range(n_band)]),
        out_shape=(jax.ShapeDtypeStruct((depth, width), bf16),) * n_band,
        in_specs=[hbm],
        out_specs=(vmem,) * n_band,
        scratch_shapes=[pltpu.SemaphoreType.DMA((n_band,))],
        compiler_params=pltpu.CompilerParams(vmem_limit_bytes=4 << 20),
        cost_estimate=pl.CostEstimate(flops=10**10, transcendentals=0, bytes_accessed=4 * depth * width * n_band),
        name="slices",
    )(pltpu.with_memory_space_constraint(spectra, pltpu.HBM))
    pixels = [send(block, k) if k else block for k, block in enumerate(blocks)]
    start, gh, gl, g3 = pl.pallas_call(
        gram_kernel,
        out_shape=(jax.ShapeDtypeStruct((K, width), f32),) + (jax.ShapeDtypeStruct((K, K), bf16),) * 3,
        in_specs=[vmem] * 3,
        out_specs=(vmem,) * 4,
        compiler_params=pltpu.CompilerParams(vmem_limit_bytes=20 << 20),
        cost_estimate=pl.CostEstimate(flops=12 * K * K * width, transcendentals=0, bytes_accessed=8 * K * width),
        name="gram",
    )(gram_inverse, abundances, duals)
    wh, wl = pl.pallas_call(
        functools.partial(weights_kernel, n_band),
        out_shape=(jax.ShapeDtypeStruct((K, n_band * depth), bf16),) * 2,
        in_specs=[vmem] * (3 + n_band),
        out_specs=(vmem,) * 2,
        scratch_shapes=[pltpu.VMEM((n_band * depth, K), f32)],
        compiler_params=pltpu.CompilerParams(vmem_limit_bytes=8 << 20),
        cost_estimate=pl.CostEstimate(flops=6 * K * K * n_band * depth, transcendentals=0, bytes_accessed=4 * K * K),
        name="weights",
    )(gh, gl, g3, *members)
    z, u, sums = pl.pallas_call(
        functools.partial(admm_kernel, n_band),
        out_shape=(
            jax.ShapeDtypeStruct((K, width), f32),
            jax.ShapeDtypeStruct((K, width), f32),
            jax.ShapeDtypeStruct((n_pix * n_band, 2, 2), f32),
        ),
        in_specs=[vmem] * (7 + n_band),
        out_specs=(vmem,) * 3,
        scratch_shapes=[
            pltpu.VMEM((n_band * depth, width), f32),
            pltpu.VMEM((K, width), f32),
            pltpu.VMEM((K, width), f32),
            pltpu.VMEM((K, width), bf16),
            pltpu.VMEM((K, width), bf16),
        ],
        compiler_params=pltpu.CompilerParams(vmem_limit_bytes=32 << 20),
        cost_estimate=pl.CostEstimate(flops=12 * K * K * width, transcendentals=0, bytes_accessed=16 * K * width),
        name="admm",
    )(start, gh, gl, wh, wl, *pixels, abundances, duals)
    everyone = lax.all_to_all(sums, ("pix", "band"), 0, 0, tiled=True)
    residual_rms = jnp.sqrt(jnp.sum(everyone, axis=0) / float(width * n_pix * n_band))
    return (z, u, residual_rms)


def solution(mesh):
    sizes = (mesh.shape["pix"], mesh.shape["band"])
    return jax.shard_map(
        functools.partial(body, sizes),
        mesh=mesh,
        in_specs=(
            P("band", "pix"),
            P("band", None),
            P(),
            P(None, ("pix", "band")),
            P(None, ("pix", "band")),
        ),
        out_specs=(P(None, ("pix", "band")), P(None, ("pix", "band")), P()),
        check_vma=False,
    )
```

```python
import functools

import jax
import jax.numpy as jnp
from jax import lax
from jax.experimental import pallas as pl
from jax.experimental.pallas import tpu as pltpu
from jax.sharding import PartitionSpec as P

B = 224
K = 512
ITERS = 2
BISECT = 6
ROWS = 8
PACK = 16
LANES = 128


def dot(left, right):
    return lax.dot_general(
        left, right, (((1,), (0,)), ((), ())), preferred_element_type=jnp.float32
    )


def dot_rows(left, right):
    return lax.dot_general(
        left, right, (((1,), (1,)), ((), ())), preferred_element_type=jnp.float32
    )


def halves(value):
    high = value.astype(jnp.bfloat16)
    return high, (value - high.astype(jnp.float32)).astype(jnp.bfloat16)


def slice_kernel(offsets, spectra_ref, *refs):
    outs, sems = refs[:-1], refs[-1]
    width = outs[0].shape[1]
    copies = []
    for i, (offset, out) in enumerate(zip(offsets(), outs)):
        columns = pl.ds(pl.multiple_of(offset * width, LANES), width)
        copies.append(pltpu.make_async_copy(spectra_ref.at[:, columns], out, sems.at[i]))
    for copy in copies:
        copy.start()
    for copy in copies:
        copy.wait()


def gram_kernel(gram_ref, z_ref, u_ref, start_ref, gh_ref, gl_ref, g3_ref):
    width = z_ref.shape[1]
    step = min(width, 256)
    gram = gram_ref[...]
    gh = gram.astype(jnp.bfloat16)
    rest = gram - gh.astype(jnp.float32)
    gl = rest.astype(jnp.bfloat16)
    gh_ref[...] = gh
    gl_ref[...] = gl
    g3_ref[...] = (rest - gl.astype(jnp.float32)).astype(jnp.bfloat16)
    for j in range(0, width, step):
        columns = slice(j, j + step)
        dual = u_ref[:, columns]
        high, low = halves(z_ref[:, columns] - dual)
        product = dot(gh_ref[...], high) + (dot(gh_ref[...], low) + dot(gl_ref[...], high))
        start_ref[:, columns] = product + dual


def weights_kernel(blocks, *refs):
    gh_ref, gl_ref, g3_ref = refs[:3]
    member_refs = refs[3 : 3 + blocks]
    wh_ref, wl_ref, rows_ref = refs[3 + blocks :]
    scale = 1.0 / (K * (B / (2.0 * K * K)))
    depth = member_refs[0].shape[0]
    for k, ref in enumerate(member_refs):
        rows_ref[k * depth : (k + 1) * depth, :] = ref[...].astype(jnp.float32)
    members = rows_ref[...].astype(jnp.bfloat16)
    weights = (dot_rows(g3_ref[...], members) + dot_rows(gl_ref[...], members)) + dot_rows(gh_ref[...], members)
    wh, wl = halves(weights * scale)
    wh_ref[...] = wh
    wl_ref[...] = wl


def mass_of(v_ref, columns, level):
    width = level.shape[1]
    wide = jnp.broadcast_to(level, (ROWS, width))
    even = jnp.zeros((ROWS, width), jnp.float32)
    odd = even
    for r in range(0, K, PACK):
        even = even + jnp.maximum(v_ref[r : r + ROWS, columns], wide)
        odd = odd + jnp.maximum(v_ref[r + ROWS : r + PACK, columns], wide)
    return jnp.sum(even + odd, axis=0, keepdims=True) - float(K) * level


def threshold(v_ref, columns):
    simplex_sum = float(K)
    total, high_end = column_stats(v_ref, columns)
    low_end = (total - simplex_sum) / simplex_sum
    mass_low = mass_of(v_ref, columns, low_end)
    mass_high = jnp.zeros_like(high_end)

    def bisect_once(unused, state):
        low_now, high_now, low_mass, high_mass = state
        middle = 0.5 * (low_now + high_now)
        mass = mass_of(v_ref, columns, middle)
        too_high = mass > simplex_sum
        return (
            jnp.where(too_high, middle, low_now),
            jnp.where(too_high, high_now, middle),
            jnp.where(too_high, mass, low_mass),
            jnp.where(too_high, high_mass, mass),
        )

    low_end, high_end, mass_low, mass_high = lax.fori_loop(
        0, BISECT, bisect_once, (low_end, high_end, mass_low, mass_high)
    )
    return low_end + (mass_low - simplex_sum) * (high_end - low_end) / (mass_low - mass_high)


def fold(value):
    total = value[:, :LANES]
    for j in range(LANES, value.shape[1], LANES):
        total = total + value[:, j : j + LANES]
    return jnp.sum(total, axis=0, keepdims=True)


def column_stats(v_ref, columns):
    block = v_ref[0:ROWS, columns]
    total = block
    top = block
    for r in range(ROWS, K, ROWS):
        block = v_ref[r : r + ROWS, columns]
        total = total + block
        top = jnp.maximum(top, block)
    return jnp.sum(total, axis=0, keepdims=True), jnp.max(top, axis=0, keepdims=True)


def admm_kernel(blocks, *refs):
    start_ref, gh_ref, gl_ref, wh_ref, wl_ref = refs[:5]
    spectra_refs = refs[5 : 5 + blocks]
    z_ref, u_ref, v2_ref, level_ref, sums_ref = refs[5 + blocks : 10 + blocks]
    rows_ref, v_ref, high_ref, low_ref = refs[10 + blocks :]
    depth = spectra_refs[0].shape[0]
    for k, ref in enumerate(spectra_refs):
        rows_ref[k * depth : (k + 1) * depth, :] = ref[...].astype(jnp.float32)
    width = v_ref.shape[1]
    half = width // 2
    step = min(half, 256)
    levels = {}
    sums = [jnp.zeros((1, LANES), jnp.float32)] * 4

    def fit(first):
        for j in range(first, first + half, step):
            columns = slice(j, j + step)
            pixels = rows_ref[:, columns].astype(jnp.bfloat16)
            v_ref[:, columns] = (dot(wl_ref[...], pixels) + dot(wh_ref[...], pixels)) + start_ref[:, columns]

    def update(first):
        columns = slice(first, first + half)
        wide = jnp.broadcast_to(levels[first], (ROWS, half))
        primal = jnp.zeros((ROWS, half), jnp.float32)
        change = primal
        for r in range(0, K, PACK):
            pieces = []
            for q in (r, r + ROWS):
                rows = slice(q, q + ROWS)
                v = v_ref[rows, columns]
                u = jnp.minimum(v, wide)
                z = v - u
                du = u - u_ref[rows, columns]
                dz = z - z_ref[rows, columns]
                primal = primal + du * du
                change = change + dz * dz
                pieces.append(z - u)
            high, low = halves(jnp.concatenate(pieces, axis=0))
            high_ref[r : r + PACK, columns] = high
            low_ref[r : r + PACK, columns] = low
        sums[0] = sums[0] + fold(primal)
        sums[2] = sums[2] + fold(change)

    def multiply(first):
        for j in range(first, first + half, step):
            columns = slice(j, j + step)
            high = high_ref[:, columns]
            product = dot(gh_ref[...], high) + (dot(gh_ref[...], low_ref[:, columns]) + dot(gl_ref[...], high))
            v = v_ref[:, columns]
            level = levels[first][:, j - first : j - first + step]
            v2_ref[:, columns] = product + ((v - start_ref[:, columns]) + jnp.minimum(v, level))

    def residuals(first):
        columns = slice(first, first + half)
        level2 = threshold(v2_ref, columns)
        wide2 = jnp.broadcast_to(level2, (ROWS, half))
        level_ref[:, columns] = wide2
        wide = jnp.broadcast_to(levels[first], (ROWS, half))
        primal = jnp.zeros((ROWS, half), jnp.float32)
        change = primal
        for r in range(0, K, ROWS):
            rows = slice(r, r + ROWS)
            v = v_ref[rows, columns]
            v2 = v2_ref[rows, columns]
            du = jnp.minimum(v2, wide2) - jnp.minimum(v, wide)
            dz = (v2 - v) - du
            primal = primal + du * du
            change = change + dz * dz
        sums[1] = sums[1] + fold(primal)
        sums[3] = sums[3] + fold(change)

    firsts = (0, half)
    for first in firsts:
        fit(first)
    for first in firsts:
        levels[first] = threshold(v_ref, slice(first, first + half))
        update(first)
        multiply(first)
    for first in firsts:
        residuals(first)
    row = lax.broadcasted_iota(jnp.int32, sums_ref.shape, 1)
    column = lax.broadcasted_iota(jnp.int32, sums_ref.shape, 2)
    table = jnp.zeros(sums_ref.shape, jnp.float32)
    for i, value in enumerate(sums):
        whole = jnp.sum(value, axis=1, keepdims=True)
        table = jnp.where((row == i // 2) & (column == i % 2), whole[None], table)
    sums_ref[...] = table


def outputs_kernel(v_ref, level_ref, z_ref, u_ref):
    wide = level_ref[...]
    for r in range(0, v_ref.shape[0], ROWS):
        rows = slice(r, r + ROWS)
        v = v_ref[rows, :]
        u = jnp.minimum(v, wide)
        u_ref[rows, :] = u
        z_ref[rows, :] = v - u


def body(sizes, spectra, endmembers, gram_inverse, abundances, duals):
    n_pix, n_band = sizes
    width = abundances.shape[1]
    depth = spectra.shape[0]

    def partner(i, k):
        return i ^ k if n_band & (n_band - 1) == 0 else (i + k) % n_band

    def send(x, k):
        return lax.ppermute(x, "band", [(i, partner(i, k)) for i in range(n_band)])

    members = [endmembers] + [None] * (n_band - 1)
    if n_band & (n_band - 1) == 0:
        stride = n_band // 2
        have = [0]
        while stride:
            for h in list(have):
                members[h ^ stride] = send(members[h], stride)
                have.append(h ^ stride)
            stride //= 2
    else:
        for k in range(1, n_band):
            members[k] = send(endmembers, k)
    vmem = pl.BlockSpec(memory_space=pltpu.VMEM)
    hbm = pl.BlockSpec(memory_space=pltpu.HBM)
    f32 = jnp.float32
    bf16 = jnp.bfloat16
    blocks = pl.pallas_call(
        functools.partial(slice_kernel, lambda: [partner(lax.axis_index("band"), k) for k in range(n_band)]),
        out_shape=(jax.ShapeDtypeStruct((depth, width), bf16),) * n_band,
        in_specs=[hbm],
        out_specs=(vmem,) * n_band,
        scratch_shapes=[pltpu.SemaphoreType.DMA((n_band,))],
        compiler_params=pltpu.CompilerParams(vmem_limit_bytes=4 << 20),
        cost_estimate=pl.CostEstimate(flops=10**10, transcendentals=0, bytes_accessed=4 * depth * width * n_band),
        name="slices",
    )(pltpu.with_memory_space_constraint(spectra, pltpu.HBM))
    pixels = list(blocks)
    for k in [*range(2, n_band), *range(1, min(2, n_band))]:
        pixels[k] = send(blocks[k], k)
    start, gh, gl, g3 = pl.pallas_call(
        gram_kernel,
        out_shape=(jax.ShapeDtypeStruct((K, width), f32),) + (jax.ShapeDtypeStruct((K, K), bf16),) * 3,
        in_specs=[vmem] * 3,
        out_specs=(vmem,) * 4,
        compiler_params=pltpu.CompilerParams(vmem_limit_bytes=20 << 20),
        cost_estimate=pl.CostEstimate(flops=12 * K * K * width, transcendentals=0, bytes_accessed=8 * K * width),
        name="gram",
    )(gram_inverse, abundances, duals)
    wh, wl = pl.pallas_call(
        functools.partial(weights_kernel, n_band),
        out_shape=(jax.ShapeDtypeStruct((K, n_band * depth), bf16),) * 2,
        in_specs=[vmem] * (3 + n_band),
        out_specs=(vmem,) * 2,
        scratch_shapes=[pltpu.VMEM((n_band * depth, K), f32)],
        compiler_params=pltpu.CompilerParams(vmem_limit_bytes=8 << 20),
        cost_estimate=pl.CostEstimate(flops=6 * K * K * n_band * depth, transcendentals=0, bytes_accessed=4 * K * K),
        name="weights",
    )(gh, gl, g3, *members)
    v, level, sums = pl.pallas_call(
        functools.partial(admm_kernel, n_band),
        out_shape=(
            jax.ShapeDtypeStruct((K, width), f32),
            jax.ShapeDtypeStruct((ROWS, width), f32),
            jax.ShapeDtypeStruct((n_pix * n_band, 2, 2), f32),
        ),
        in_specs=[vmem] * (7 + n_band),
        out_specs=(vmem,) * 3,
        scratch_shapes=[
            pltpu.VMEM((n_band * depth, width), f32),
            pltpu.VMEM((K, width), f32),
            pltpu.VMEM((K, width), bf16),
            pltpu.VMEM((K, width), bf16),
        ],
        compiler_params=pltpu.CompilerParams(vmem_limit_bytes=24 << 20),
        cost_estimate=pl.CostEstimate(flops=12 * K * K * width, transcendentals=0, bytes_accessed=16 * K * width),
        name="admm",
    )(start, gh, gl, wh, wl, *pixels, abundances, duals)
    part = K // 4
    wide_spec = pl.BlockSpec((part, width), lambda i: (i, 0))
    z, u = pl.pallas_call(
        outputs_kernel,
        out_shape=(jax.ShapeDtypeStruct((K, width), f32),) * 2,
        grid=(K // part,),
        in_specs=[wide_spec, pl.BlockSpec((ROWS, width), lambda i: (0, 0))],
        out_specs=(wide_spec,) * 2,
        compiler_params=pltpu.CompilerParams(vmem_limit_bytes=8 << 20),
        cost_estimate=pl.CostEstimate(flops=K * K * width, transcendentals=0, bytes_accessed=8 * K * width),
        name="outputs",
    )(v, level)
    everyone = lax.all_to_all(sums, ("pix", "band"), 0, 0, tiled=True)
    residual_rms = jnp.sqrt(jnp.sum(everyone, axis=0) / float(width * n_pix * n_band))
    return (z, u, residual_rms)


def solution(mesh):
    sizes = (mesh.shape["pix"], mesh.shape["band"])
    return jax.shard_map(
        functools.partial(body, sizes),
        mesh=mesh,
        in_specs=(
            P("band", "pix"),
            P("band", None),
            P(),
            P(None, ("pix", "band")),
            P(None, ("pix", "band")),
        ),
        out_specs=(P(None, ("pix", "band")), P(None, ("pix", "band")), P()),
        check_vma=False,
    )
```

```python
import functools

import jax
import jax.numpy as jnp
from jax import lax
from jax.experimental import pallas as pl
from jax.experimental.pallas import tpu as pltpu
from jax.sharding import PartitionSpec as P

B = 224
K = 512
ITERS = 2
BISECT = 6
ROWS = 8
PACK = 16
LANES = 128


def dot(left, right):
    return lax.dot_general(
        left, right, (((1,), (0,)), ((), ())), preferred_element_type=jnp.float32
    )


def dot_rows(left, right):
    return lax.dot_general(
        left, right, (((1,), (1,)), ((), ())), preferred_element_type=jnp.float32
    )


def halves(value):
    high = value.astype(jnp.bfloat16)
    return high, (value - high.astype(jnp.float32)).astype(jnp.bfloat16)


def slice_kernel(offsets, spectra_ref, *refs):
    outs, sems = refs[:-1], refs[-1]
    width = outs[0].shape[1]
    copies = []
    for i, (offset, out) in enumerate(zip(offsets(), outs)):
        columns = pl.ds(pl.multiple_of(offset * width, LANES), width)
        copies.append(pltpu.make_async_copy(spectra_ref.at[:, columns], out, sems.at[i]))
    for copy in copies:
        copy.start()
    for copy in copies:
        copy.wait()


def gram_kernel(gram_ref, z_ref, u_ref, start_ref, gh_ref, gl_ref, g3_ref):
    width = z_ref.shape[1]
    step = min(width, 256)
    gram = gram_ref[...]
    gh = gram.astype(jnp.bfloat16)
    rest = gram - gh.astype(jnp.float32)
    gl = rest.astype(jnp.bfloat16)
    gh_ref[...] = gh
    gl_ref[...] = gl
    g3_ref[...] = (rest - gl.astype(jnp.float32)).astype(jnp.bfloat16)
    for j in range(0, width, step):
        columns = slice(j, j + step)
        dual = u_ref[:, columns]
        high, low = halves(z_ref[:, columns] - dual)
        product = dot(gh_ref[...], high) + (dot(gh_ref[...], low) + dot(gl_ref[...], high))
        start_ref[:, columns] = product + dual


def weights_kernel(blocks, *refs):
    gh_ref, gl_ref, g3_ref = refs[:3]
    member_refs = refs[3 : 3 + blocks]
    wh_ref, wl_ref, rows_ref = refs[3 + blocks :]
    scale = 1.0 / (K * (B / (2.0 * K * K)))
    depth = member_refs[0].shape[0]
    for k, ref in enumerate(member_refs):
        rows_ref[k * depth : (k + 1) * depth, :] = ref[...].astype(jnp.float32)
    members = rows_ref[...].astype(jnp.bfloat16)
    weights = (dot_rows(g3_ref[...], members) + dot_rows(gl_ref[...], members)) + dot_rows(gh_ref[...], members)
    wh, wl = halves(weights * scale)
    wh_ref[...] = wh
    wl_ref[...] = wl


def mass_of(v_ref, columns, level):
    width = level.shape[1]
    wide = jnp.broadcast_to(level, (ROWS, width))
    even = jnp.zeros((ROWS, width), jnp.float32)
    odd = even
    for r in range(0, K, PACK):
        even = even + jnp.maximum(v_ref[r : r + ROWS, columns], wide)
        odd = odd + jnp.maximum(v_ref[r + ROWS : r + PACK, columns], wide)
    return jnp.sum(even + odd, axis=0, keepdims=True) - float(K) * level


def threshold(v_ref, columns):
    simplex_sum = float(K)
    total, high_end = column_stats(v_ref, columns)
    low_end = (total - simplex_sum) / simplex_sum
    mass_low = mass_of(v_ref, columns, low_end)
    mass_high = jnp.zeros_like(high_end)

    def bisect_once(unused, state):
        low_now, high_now, low_mass, high_mass = state
        middle = 0.5 * (low_now + high_now)
        mass = mass_of(v_ref, columns, middle)
        too_high = mass > simplex_sum
        return (
            jnp.where(too_high, middle, low_now),
            jnp.where(too_high, high_now, middle),
            jnp.where(too_high, mass, low_mass),
            jnp.where(too_high, high_mass, mass),
        )

    low_end, high_end, mass_low, mass_high = lax.fori_loop(
        0, BISECT, bisect_once, (low_end, high_end, mass_low, mass_high)
    )
    return low_end + (mass_low - simplex_sum) * (high_end - low_end) / (mass_low - mass_high)


def fold(value):
    total = value[:, :LANES]
    for j in range(LANES, value.shape[1], LANES):
        total = total + value[:, j : j + LANES]
    return jnp.sum(total, axis=0, keepdims=True)


def column_stats(v_ref, columns):
    block = v_ref[0:ROWS, columns]
    total = block
    top = block
    for r in range(ROWS, K, ROWS):
        block = v_ref[r : r + ROWS, columns]
        total = total + block
        top = jnp.maximum(top, block)
    return jnp.sum(total, axis=0, keepdims=True), jnp.max(top, axis=0, keepdims=True)


def admm_kernel(blocks, *refs):
    start_ref, gh_ref, gl_ref, wh_ref, wl_ref = refs[:5]
    spectra_refs = refs[5 : 5 + blocks]
    z_ref, u_ref, v2_ref, level_ref, sums_ref = refs[5 + blocks : 10 + blocks]
    rows_ref, v_ref, high_ref, low_ref = refs[10 + blocks :]
    depth = spectra_refs[0].shape[0]
    for k, ref in enumerate(spectra_refs):
        rows_ref[k * depth : (k + 1) * depth, :] = ref[...].astype(jnp.float32)
    width = v_ref.shape[1]
    half = width // 2
    step = min(half, 256)
    levels = {}
    sums = [jnp.zeros((1, LANES), jnp.float32)] * 4

    def fit(first):
        for j in range(first, first + half, step):
            columns = slice(j, j + step)
            pixels = rows_ref[:, columns].astype(jnp.bfloat16)
            v_ref[:, columns] = (dot(wl_ref[...], pixels) + dot(wh_ref[...], pixels)) + start_ref[:, columns]

    def update(first):
        columns = slice(first, first + half)
        wide = jnp.broadcast_to(levels[first], (ROWS, half))
        primal = jnp.zeros((ROWS, half), jnp.float32)
        change = primal
        for r in range(0, K, PACK):
            pieces = []
            for q in (r, r + ROWS):
                rows = slice(q, q + ROWS)
                v = v_ref[rows, columns]
                u = jnp.minimum(v, wide)
                z = v - u
                du = u - u_ref[rows, columns]
                dz = z - z_ref[rows, columns]
                primal = primal + du * du
                change = change + dz * dz
                pieces.append(z - u)
            high, low = halves(jnp.concatenate(pieces, axis=0))
            high_ref[r : r + PACK, columns] = high
            low_ref[r : r + PACK, columns] = low
        sums[0] = sums[0] + fold(primal)
        sums[2] = sums[2] + fold(change)

    def multiply(first):
        for j in range(first, first + half, step):
            columns = slice(j, j + step)
            high = high_ref[:, columns]
            product = dot(gh_ref[...], high) + (dot(gh_ref[...], low_ref[:, columns]) + dot(gl_ref[...], high))
            v = v_ref[:, columns]
            level = levels[first][:, j - first : j - first + step]
            v2_ref[:, columns] = product + ((v - start_ref[:, columns]) + jnp.minimum(v, level))

    def residuals(first):
        columns = slice(first, first + half)
        level2 = threshold(v2_ref, columns)
        wide2 = jnp.broadcast_to(level2, (ROWS, half))
        level_ref[:, columns] = wide2
        wide = jnp.broadcast_to(levels[first], (ROWS, half))
        primal = jnp.zeros((ROWS, half), jnp.float32)
        change = primal
        for r in range(0, K, ROWS):
            rows = slice(r, r + ROWS)
            v = v_ref[rows, columns]
            v2 = v2_ref[rows, columns]
            du = jnp.minimum(v2, wide2) - jnp.minimum(v, wide)
            dz = (v2 - v) - du
            primal = primal + du * du
            change = change + dz * dz
        sums[1] = sums[1] + fold(primal)
        sums[3] = sums[3] + fold(change)

    firsts = (0, half)
    for first in firsts:
        fit(first)
    for first in firsts:
        levels[first] = threshold(v_ref, slice(first, first + half))
        update(first)
        multiply(first)
    for first in firsts:
        residuals(first)
    row = lax.broadcasted_iota(jnp.int32, sums_ref.shape, 1)
    column = lax.broadcasted_iota(jnp.int32, sums_ref.shape, 2)
    table = jnp.zeros(sums_ref.shape, jnp.float32)
    for i, value in enumerate(sums):
        whole = jnp.sum(value, axis=1, keepdims=True)
        table = jnp.where((row == i // 2) & (column == i % 2), whole[None], table)
    sums_ref[...] = table


def outputs_kernel(v_ref, level_ref, z_ref, u_ref):
    wide = level_ref[...]
    for r in range(0, v_ref.shape[0], ROWS):
        rows = slice(r, r + ROWS)
        v = v_ref[rows, :]
        u = jnp.minimum(v, wide)
        u_ref[rows, :] = u
        z_ref[rows, :] = v - u


def body(sizes, spectra, endmembers, gram_inverse, abundances, duals):
    n_pix, n_band = sizes
    width = abundances.shape[1]
    depth = spectra.shape[0]

    def partner(i, k):
        return i ^ k if n_band & (n_band - 1) == 0 else (i + k) % n_band

    def send(x, k):
        return lax.ppermute(x, "band", [(i, partner(i, k)) for i in range(n_band)])

    vmem = pl.BlockSpec(memory_space=pltpu.VMEM)
    hbm = pl.BlockSpec(memory_space=pltpu.HBM)
    f32 = jnp.float32
    bf16 = jnp.bfloat16
    blocks = pl.pallas_call(
        functools.partial(slice_kernel, lambda: [partner(lax.axis_index("band"), k) for k in range(n_band)]),
        out_shape=(jax.ShapeDtypeStruct((depth, width), bf16),) * n_band,
        in_specs=[hbm],
        out_specs=(vmem,) * n_band,
        scratch_shapes=[pltpu.SemaphoreType.DMA((n_band,))],
        compiler_params=pltpu.CompilerParams(vmem_limit_bytes=4 << 20),
        cost_estimate=pl.CostEstimate(flops=10**10, transcendentals=0, bytes_accessed=4 * depth * width * n_band),
        name="slices",
    )(pltpu.with_memory_space_constraint(spectra, pltpu.HBM))
    pixels = list(blocks)
    members = [endmembers] + [None] * (n_band - 1)
    doubling = n_band & (n_band - 1) == 0
    stride = n_band // 2 if doubling and n_band > 2 else 0
    if stride:
        members[stride] = send(endmembers, stride)
    for k in range(2, n_band):
        pixels[k] = send(blocks[k], k)
    late = (endmembers, *blocks[1:2])
    if stride:
        late = lax.optimization_barrier((*late, members[stride]))
    if n_band > 1:
        pixels[1] = send(late[1], 1)
    have = [0, stride] if stride else [0]
    stride = stride // 2 if stride else 1
    while doubling and stride < n_band and stride:
        for h in list(have):
            members[h ^ stride] = send(members[h] if h else late[0], stride)
            have.append(h ^ stride)
        stride //= 2
    if not doubling:
        for k in range(1, n_band):
            members[k] = send(endmembers, k)
    start, gh, gl, g3 = pl.pallas_call(
        gram_kernel,
        out_shape=(jax.ShapeDtypeStruct((K, width), f32),) + (jax.ShapeDtypeStruct((K, K), bf16),) * 3,
        in_specs=[vmem] * 3,
        out_specs=(vmem,) * 4,
        compiler_params=pltpu.CompilerParams(vmem_limit_bytes=20 << 20),
        cost_estimate=pl.CostEstimate(flops=12 * K * K * width, transcendentals=0, bytes_accessed=8 * K * width),
        name="gram",
    )(gram_inverse, abundances, duals)
    wh, wl = pl.pallas_call(
        functools.partial(weights_kernel, n_band),
        out_shape=(jax.ShapeDtypeStruct((K, n_band * depth), bf16),) * 2,
        in_specs=[vmem] * (3 + n_band),
        out_specs=(vmem,) * 2,
        scratch_shapes=[pltpu.VMEM((n_band * depth, K), f32)],
        compiler_params=pltpu.CompilerParams(vmem_limit_bytes=8 << 20),
        cost_estimate=pl.CostEstimate(flops=6 * K * K * n_band * depth, transcendentals=0, bytes_accessed=4 * K * K),
        name="weights",
    )(gh, gl, g3, *members)
    v, level, sums = pl.pallas_call(
        functools.partial(admm_kernel, n_band),
        out_shape=(
            jax.ShapeDtypeStruct((K, width), f32),
            jax.ShapeDtypeStruct((ROWS, width), f32),
            jax.ShapeDtypeStruct((n_pix * n_band, 2, 2), f32),
        ),
        in_specs=[vmem] * (7 + n_band),
        out_specs=(vmem,) * 3,
        scratch_shapes=[
            pltpu.VMEM((n_band * depth, width), f32),
            pltpu.VMEM((K, width), f32),
            pltpu.VMEM((K, width), bf16),
            pltpu.VMEM((K, width), bf16),
        ],
        compiler_params=pltpu.CompilerParams(vmem_limit_bytes=24 << 20),
        cost_estimate=pl.CostEstimate(flops=12 * K * K * width, transcendentals=0, bytes_accessed=16 * K * width),
        name="admm",
    )(start, gh, gl, wh, wl, *pixels, abundances, duals)
    part = K // 4
    wide_spec = pl.BlockSpec((part, width), lambda i: (i, 0))
    z, u = pl.pallas_call(
        outputs_kernel,
        out_shape=(jax.ShapeDtypeStruct((K, width), f32),) * 2,
        grid=(K // part,),
        in_specs=[wide_spec, pl.BlockSpec((ROWS, width), lambda i: (0, 0))],
        out_specs=(wide_spec,) * 2,
        compiler_params=pltpu.CompilerParams(vmem_limit_bytes=8 << 20),
        cost_estimate=pl.CostEstimate(flops=K * K * width, transcendentals=0, bytes_accessed=8 * K * width),
        name="outputs",
    )(v, level)
    everyone = lax.all_to_all(sums, ("pix", "band"), 0, 0, tiled=True)
    residual_rms = jnp.sqrt(jnp.sum(everyone, axis=0) / float(width * n_pix * n_band))
    return (z, u, residual_rms)


def solution(mesh):
    sizes = (mesh.shape["pix"], mesh.shape["band"])
    return jax.shard_map(
        functools.partial(body, sizes),
        mesh=mesh,
        in_specs=(
            P("band", "pix"),
            P("band", None),
            P(),
            P(None, ("pix", "band")),
            P(None, ("pix", "band")),
        ),
        out_specs=(P(None, ("pix", "band")), P(None, ("pix", "band")), P()),
        check_vma=False,
    )
```

```python
import functools

import jax
import jax.numpy as jnp
from jax import lax
from jax.experimental import pallas as pl
from jax.experimental.pallas import tpu as pltpu
from jax.sharding import PartitionSpec as P

B = 224
K = 512
ITERS = 2
BISECT = 6
ROWS = 8
PACK = 16
LANES = 128


def dot(left, right):
    return lax.dot_general(
        left, right, (((1,), (0,)), ((), ())), preferred_element_type=jnp.float32
    )


def dot_rows(left, right):
    return lax.dot_general(
        left, right, (((1,), (1,)), ((), ())), preferred_element_type=jnp.float32
    )


def halves(value):
    high = value.astype(jnp.bfloat16)
    return high, (value - high.astype(jnp.float32)).astype(jnp.bfloat16)


def slice_kernel(offsets, spectra_ref, *refs):
    outs, sems = refs[:-1], refs[-1]
    width = outs[0].shape[1]
    copies = []
    for i, (offset, out) in enumerate(zip(offsets(), outs)):
        columns = pl.ds(pl.multiple_of(offset * width, LANES), width)
        copies.append(pltpu.make_async_copy(spectra_ref.at[:, columns], out, sems.at[i]))
    for copy in copies:
        copy.start()
    for copy in copies:
        copy.wait()


def gram_kernel(gram_ref, z_ref, u_ref, start_ref, gh_ref, gl_ref, g3_ref):
    width = z_ref.shape[1]
    step = min(width, 256)
    gram = gram_ref[...]
    gh = gram.astype(jnp.bfloat16)
    rest = gram - gh.astype(jnp.float32)
    gl = rest.astype(jnp.bfloat16)
    gh_ref[...] = gh
    gl_ref[...] = gl
    g3_ref[...] = (rest - gl.astype(jnp.float32)).astype(jnp.bfloat16)
    for j in range(0, width, step):
        columns = slice(j, j + step)
        dual = u_ref[:, columns]
        high, low = halves(z_ref[:, columns] - dual)
        product = dot(gh_ref[...], high) + (dot(gh_ref[...], low) + dot(gl_ref[...], high))
        start_ref[:, columns] = product + dual


def weights_kernel(blocks, *refs):
    gh_ref, gl_ref, g3_ref = refs[:3]
    member_refs = refs[3 : 3 + blocks]
    wh_ref, wl_ref, rows_ref = refs[3 + blocks :]
    scale = 1.0 / (K * (B / (2.0 * K * K)))
    depth = member_refs[0].shape[0]
    for k, ref in enumerate(member_refs):
        rows_ref[k * depth : (k + 1) * depth, :] = ref[...].astype(jnp.float32)
    members = rows_ref[...].astype(jnp.bfloat16)
    weights = (dot_rows(g3_ref[...], members) + dot_rows(gl_ref[...], members)) + dot_rows(gh_ref[...], members)
    wh, wl = halves(weights * scale)
    wh_ref[...] = wh
    wl_ref[...] = wl


def mass_of(v_ref, columns, level):
    width = level.shape[1]
    wide = jnp.broadcast_to(level, (ROWS, width))
    even = jnp.zeros((ROWS, width), jnp.float32)
    odd = even
    for r in range(0, K, PACK):
        even = even + jnp.maximum(v_ref[r : r + ROWS, columns], wide)
        odd = odd + jnp.maximum(v_ref[r + ROWS : r + PACK, columns], wide)
    return jnp.sum(even + odd, axis=0, keepdims=True) - float(K) * level


def threshold(v_ref, columns, stats):
    simplex_sum = float(K)
    total = jnp.concatenate([s for s, _ in stats], axis=1)
    high_end = jnp.concatenate([t for _, t in stats], axis=1)
    low_end = (total - simplex_sum) / simplex_sum
    mass_low = mass_of(v_ref, columns, low_end)
    mass_high = jnp.zeros_like(high_end)

    def bisect_once(unused, state):
        low_now, high_now, low_mass, high_mass = state
        middle = 0.5 * (low_now + high_now)
        mass = mass_of(v_ref, columns, middle)
        too_high = mass > simplex_sum
        return (
            jnp.where(too_high, middle, low_now),
            jnp.where(too_high, high_now, middle),
            jnp.where(too_high, mass, low_mass),
            jnp.where(too_high, high_mass, mass),
        )

    low_end, high_end, mass_low, mass_high = lax.fori_loop(
        0, BISECT, bisect_once, (low_end, high_end, mass_low, mass_high)
    )
    return low_end + (mass_low - simplex_sum) * (high_end - low_end) / (mass_low - mass_high)


def fold(value):
    total = value[:, :LANES]
    for j in range(LANES, value.shape[1], LANES):
        total = total + value[:, j : j + LANES]
    return jnp.sum(total, axis=0, keepdims=True)


def column_stats(value):
    return jnp.sum(value, axis=0, keepdims=True), jnp.max(value, axis=0, keepdims=True)


def admm_kernel(blocks, *refs):
    start_ref, gh_ref, gl_ref, wh_ref, wl_ref = refs[:5]
    spectra_refs = refs[5 : 5 + blocks]
    z_ref, u_ref, v2_ref, level_ref, sums_ref = refs[5 + blocks : 10 + blocks]
    rows_ref, v_ref, high_ref, low_ref = refs[10 + blocks :]
    depth = spectra_refs[0].shape[0]
    for k, ref in enumerate(spectra_refs):
        rows_ref[k * depth : (k + 1) * depth, :] = ref[...].astype(jnp.float32)
    width = v_ref.shape[1]
    half = width // 2
    step = min(half, 256)
    levels = {}
    stats = {0: [], half: []}
    stats2 = {0: [], half: []}
    sums = [jnp.zeros((1, LANES), jnp.float32)] * 4

    def fit(first):
        for j in range(first, first + half, step):
            columns = slice(j, j + step)
            pixels = rows_ref[:, columns].astype(jnp.bfloat16)
            value = (dot(wl_ref[...], pixels) + dot(wh_ref[...], pixels)) + start_ref[:, columns]
            v_ref[:, columns] = value
            stats[first].append(column_stats(value))

    def update(first):
        columns = slice(first, first + half)
        wide = jnp.broadcast_to(levels[first], (ROWS, half))
        primal = jnp.zeros((ROWS, half), jnp.float32)
        change = primal
        for r in range(0, K, PACK):
            pieces = []
            for q in (r, r + ROWS):
                rows = slice(q, q + ROWS)
                v = v_ref[rows, columns]
                u = jnp.minimum(v, wide)
                z = v - u
                du = u - u_ref[rows, columns]
                dz = z - z_ref[rows, columns]
                primal = primal + du * du
                change = change + dz * dz
                pieces.append(z - u)
            high, low = halves(jnp.concatenate(pieces, axis=0))
            high_ref[r : r + PACK, columns] = high
            low_ref[r : r + PACK, columns] = low
        sums[0] = sums[0] + fold(primal)
        sums[2] = sums[2] + fold(change)

    def multiply(first):
        for j in range(first, first + half, step):
            columns = slice(j, j + step)
            high = high_ref[:, columns]
            product = dot(gh_ref[...], high) + (dot(gh_ref[...], low_ref[:, columns]) + dot(gl_ref[...], high))
            v = v_ref[:, columns]
            level = levels[first][:, j - first : j - first + step]
            value = product + ((v - start_ref[:, columns]) + jnp.minimum(v, level))
            v2_ref[:, columns] = value
            stats2[first].append(column_stats(value))

    def residuals(first):
        columns = slice(first, first + half)
        wide2 = jnp.broadcast_to(levels2[first], (ROWS, half))
        level_ref[:, columns] = wide2
        wide = jnp.broadcast_to(levels[first], (ROWS, half))
        primal = jnp.zeros((ROWS, half), jnp.float32)
        change = primal
        for r in range(0, K, ROWS):
            rows = slice(r, r + ROWS)
            v = v_ref[rows, columns]
            v2 = v2_ref[rows, columns]
            du = jnp.minimum(v2, wide2) - jnp.minimum(v, wide)
            dz = (v2 - v) - du
            primal = primal + du * du
            change = change + dz * dz
        sums[1] = sums[1] + fold(primal)
        sums[3] = sums[3] + fold(change)

    firsts = (0, half)
    for first in firsts:
        fit(first)
    for first in firsts:
        levels[first] = threshold(v_ref, slice(first, first + half), stats[first])
    for first in firsts:
        update(first)
        multiply(first)
    levels2 = {first: threshold(v2_ref, slice(first, first + half), stats2[first]) for first in firsts}
    for first in firsts:
        residuals(first)
    row = lax.broadcasted_iota(jnp.int32, sums_ref.shape, 1)
    column = lax.broadcasted_iota(jnp.int32, sums_ref.shape, 2)
    table = jnp.zeros(sums_ref.shape, jnp.float32)
    for i, value in enumerate(sums):
        whole = jnp.sum(value, axis=1, keepdims=True)
        table = jnp.where((row == i // 2) & (column == i % 2), whole[None], table)
    sums_ref[...] = table


def outputs_kernel(v_ref, level_ref, z_ref, u_ref):
    wide = level_ref[...]
    for r in range(0, v_ref.shape[0], ROWS):
        rows = slice(r, r + ROWS)
        v = v_ref[rows, :]
        u = jnp.minimum(v, wide)
        u_ref[rows, :] = u
        z_ref[rows, :] = v - u


def body(sizes, spectra, endmembers, gram_inverse, abundances, duals):
    n_pix, n_band = sizes
    width = abundances.shape[1]
    depth = spectra.shape[0]

    def partner(i, k):
        return i ^ k if n_band & (n_band - 1) == 0 else (i + k) % n_band

    def send(x, k):
        return lax.ppermute(x, "band", [(i, partner(i, k)) for i in range(n_band)])

    vmem = pl.BlockSpec(memory_space=pltpu.VMEM)
    hbm = pl.BlockSpec(memory_space=pltpu.HBM)
    f32 = jnp.float32
    bf16 = jnp.bfloat16
    blocks = pl.pallas_call(
        functools.partial(slice_kernel, lambda: [partner(lax.axis_index("band"), k) for k in range(n_band)]),
        out_shape=(jax.ShapeDtypeStruct((depth, width), bf16),) * n_band,
        in_specs=[hbm],
        out_specs=(vmem,) * n_band,
        scratch_shapes=[pltpu.SemaphoreType.DMA((n_band,))],
        compiler_params=pltpu.CompilerParams(vmem_limit_bytes=4 << 20),
        cost_estimate=pl.CostEstimate(flops=10**10, transcendentals=0, bytes_accessed=4 * depth * width * n_band),
        name="slices",
    )(pltpu.with_memory_space_constraint(spectra, pltpu.HBM))
    pixels = list(blocks)
    members = [endmembers] + [None] * (n_band - 1)
    doubling = n_band & (n_band - 1) == 0
    stride = n_band // 2 if doubling and n_band > 2 else 0
    if stride:
        members[stride] = send(endmembers, stride)
    for k in range(2, n_band):
        pixels[k] = send(blocks[k], k)
    late = (endmembers, *blocks[1:2])
    if stride:
        late = lax.optimization_barrier((*late, members[stride]))
    if n_band > 1:
        pixels[1] = send(late[1], 1)
    have = [0, stride] if stride else [0]
    stride = stride // 2 if stride else 1
    while doubling and stride < n_band and stride:
        for h in list(have):
            members[h ^ stride] = send(members[h] if h else late[0], stride)
            have.append(h ^ stride)
        stride //= 2
    if not doubling:
        for k in range(1, n_band):
            members[k] = send(endmembers, k)
    start, gh, gl, g3 = pl.pallas_call(
        gram_kernel,
        out_shape=(jax.ShapeDtypeStruct((K, width), f32),) + (jax.ShapeDtypeStruct((K, K), bf16),) * 3,
        in_specs=[vmem] * 3,
        out_specs=(vmem,) * 4,
        compiler_params=pltpu.CompilerParams(vmem_limit_bytes=20 << 20),
        cost_estimate=pl.CostEstimate(flops=12 * K * K * width, transcendentals=0, bytes_accessed=8 * K * width),
        name="gram",
    )(gram_inverse, abundances, duals)
    wh, wl = pl.pallas_call(
        functools.partial(weights_kernel, n_band),
        out_shape=(jax.ShapeDtypeStruct((K, n_band * depth), bf16),) * 2,
        in_specs=[vmem] * (3 + n_band),
        out_specs=(vmem,) * 2,
        scratch_shapes=[pltpu.VMEM((n_band * depth, K), f32)],
        compiler_params=pltpu.CompilerParams(vmem_limit_bytes=8 << 20),
        cost_estimate=pl.CostEstimate(flops=6 * K * K * n_band * depth, transcendentals=0, bytes_accessed=4 * K * K),
        name="weights",
    )(gh, gl, g3, *members)
    v, level, sums = pl.pallas_call(
        functools.partial(admm_kernel, n_band),
        out_shape=(
            jax.ShapeDtypeStruct((K, width), f32),
            jax.ShapeDtypeStruct((ROWS, width), f32),
            jax.ShapeDtypeStruct((n_pix * n_band, 2, 2), f32),
        ),
        in_specs=[vmem] * (7 + n_band),
        out_specs=(vmem,) * 3,
        scratch_shapes=[
            pltpu.VMEM((n_band * depth, width), f32),
            pltpu.VMEM((K, width), f32),
            pltpu.VMEM((K, width), bf16),
            pltpu.VMEM((K, width), bf16),
        ],
        compiler_params=pltpu.CompilerParams(vmem_limit_bytes=24 << 20),
        cost_estimate=pl.CostEstimate(flops=12 * K * K * width, transcendentals=0, bytes_accessed=16 * K * width),
        name="admm",
    )(start, gh, gl, wh, wl, *pixels, abundances, duals)
    part = K // 4
    wide_spec = pl.BlockSpec((part, width), lambda i: (i, 0))
    z, u = pl.pallas_call(
        outputs_kernel,
        out_shape=(jax.ShapeDtypeStruct((K, width), f32),) * 2,
        grid=(K // part,),
        in_specs=[wide_spec, pl.BlockSpec((ROWS, width), lambda i: (0, 0))],
        out_specs=(wide_spec,) * 2,
        compiler_params=pltpu.CompilerParams(vmem_limit_bytes=8 << 20),
        cost_estimate=pl.CostEstimate(flops=K * K * width, transcendentals=0, bytes_accessed=8 * K * width),
        name="outputs",
    )(v, level)
    everyone = lax.all_to_all(sums, ("pix", "band"), 0, 0, tiled=True)
    residual_rms = jnp.sqrt(jnp.sum(everyone, axis=0) / float(width * n_pix * n_band))
    return (z, u, residual_rms)


def solution(mesh):
    sizes = (mesh.shape["pix"], mesh.shape["band"])
    return jax.shard_map(
        functools.partial(body, sizes),
        mesh=mesh,
        in_specs=(
            P("band", "pix"),
            P("band", None),
            P(),
            P(None, ("pix", "band")),
            P(None, ("pix", "band")),
        ),
        out_specs=(P(None, ("pix", "band")), P(None, ("pix", "band")), P()),
        check_vma=False,
    )
```
